256 devices in a mesh: seq: 32 (over x, z_hi, core), grp: 8 (over y, z_lo).
Axes of the slice: x: 4, y: 4, z: 8 (z_hi: 4, z_lo: 2; z = z_hi * 2 + z_lo), core: 2. Of those that a mesh axis runs over, the one named last changes fastest.
Arguments:
- out_grad: bfloat16 [8, 6912, 1024], P('grp', 'seq'), may hold values from -6 to 6
- combine_logits: float32 [8, 6912, 128], P('grp', 'seq'), may hold values from -20 to 330
- expert_out: bfloat16 [8, 128, 1024], P('grp', 'seq'), may hold values from -6 to 6
- slot_in: bfloat16 [8, 128, 1024], P('grp', 'seq'), may hold values from -6 to 6
- router: bfloat16 [128, 1024], P('seq'), may hold values from -0.1875 to 0.1875
- w_gate: bfloat16 [128, 2048, 1024], P('seq', 'grp'), may hold values from -0.1875 to 0.1875
- w_up: bfloat16 [128, 2048, 1024], P('seq', 'grp'), may hold values from -0.1875 to 0.1875
- w_down: bfloat16 [128, 2048, 1024], P('seq', 'grp'), may hold values from -0.125 to 0.125
Outputs:
- token_grad: bfloat16 [8, 6912, 1024], P('grp', 'seq')
- slot_grad: float32 [8, 128, 1024], P('grp', 'seq')
- grad_gate: bfloat16 [128, 2048, 1024], P('seq', 'grp')
- grad_up: bfloat16 [128, 2048, 1024], P('seq', 'grp')
- grad_down: bfloat16 [128, 2048, 1024], P('seq', 'grp')
The draws below stay inside these ranges and needn't reach their ends.
All inputs are finite; a program needn't handle non-finite values.
Results may differ from the reference program's by a relative error of at most 0.028.
Values may be sent and summed in bfloat16 or wider, within the bound.
A program may use at most 64 MiB of HBM per device.

```python
import jax
import jax.numpy as jnp
from jax import lax

D = 1024
FF = 2048
EXPERTS = 128
TOKENS = 6912
SEQS = 8


def draw_combine_logits(key, part):
    keys = jax.random.split(key, 1)
    shape = (SEQS, TOKENS, EXPERTS)
    return jnp.clip(3.0 * jax.random.normal(keys[0], shape, jnp.float32), -18.0, 18.0)


def shard_levels(stream_key, shape, cuts, least, top_value):
    loudness = 1.0
    for dim, blocks in cuts:
        draws = jax.random.uniform(jax.random.fold_in(jax.random.fold_in(stream_key, 6), dim), (blocks,), jnp.float32, least / len(cuts), top_value / len(cuts))
        loudness = loudness * jnp.repeat(jnp.exp(draws), shape[dim] // blocks).reshape((-1,) + (1,) * (len(shape) - 1 - dim))
    return loudness


def centred(key, shape, spread, limit, cuts=(), kind=jnp.bfloat16):
    result = spread * jax.random.normal(key, shape, jnp.float32)
    if cuts:
        result = result * shard_levels(key, shape, cuts, -0.22, 0.18)
    return jnp.clip(result, -limit, limit).astype(kind)


def setup_inputs(seed: int = 0) -> dict:
    seeds = jax.random.split(jax.random.key(seed), 9)
    out_grad = centred(seeds[0], (SEQS, TOKENS, D), 1.0, 6.0, ((0, 8), (1, 32)))
    combine_logits = draw_combine_logits(jax.random.fold_in(seeds[8], 71), 0)
    expert_out = centred(seeds[2], (SEQS, EXPERTS, D), 1.0, 6.0, ((0, 8), (1, 32)))
    slot_in = centred(seeds[3], (SEQS, EXPERTS, D), 1.0, 6.0, ((0, 8), (1, 32)))
    router = centred(seeds[4], (EXPERTS, D), D ** -0.5, 0.1875, ((0, 32),))
    w_gate = centred(seeds[5], (EXPERTS, FF, D), D ** -0.5, 0.1875, ((0, 32), (1, 8)))
    w_up = centred(seeds[6], (EXPERTS, FF, D), D ** -0.5, 0.1875, ((0, 32), (1, 8)))
    w_down = centred(seeds[7], (EXPERTS, FF, D), FF ** -0.5, 0.125, ((0, 32), (1, 8)))
    return dict(out_grad=out_grad, combine_logits=combine_logits, expert_out=expert_out, slot_in=slot_in, router=router, w_gate=w_gate, w_up=w_up, w_down=w_down)


def sequence_part(items, router):
    grads, logits, outputs = items
    probs = jax.nn.softmax(logits, axis=-1)
    probs_bf = probs.astype(jnp.bfloat16)
    slot_out = lax.dot_general(probs_bf, grads, (((0,), (0,)), ((), ())), preferred_element_type=jnp.float32)
    weight_grad = lax.dot_general(grads, outputs, (((1,), (1,)), ((), ())), preferred_element_type=jnp.float32)
    centre = jnp.sum(weight_grad * probs, axis=-1, keepdims=True)
    logit_grad = (probs * (weight_grad - centre)).astype(jnp.bfloat16)
    token_grad = jnp.dot(logit_grad, router, preferred_element_type=jnp.float32).astype(jnp.bfloat16)
    return token_grad, slot_out.astype(jnp.bfloat16)


def expert_part(items):
    inputs, out_grads, w_gate, w_up, w_down = items
    dims = (((1,), (1,)), ((), ()))
    gate = lax.dot_general(inputs, w_gate, dims, preferred_element_type=jnp.float32)
    upper = lax.dot_general(inputs, w_up, dims, preferred_element_type=jnp.float32)
    sig = jax.nn.sigmoid(gate)
    hidden = (gate * sig * upper).astype(jnp.bfloat16)
    hidden_grad = lax.dot_general(out_grads, w_down, dims, preferred_element_type=jnp.float32)
    up_grad = (hidden_grad * gate * sig).astype(jnp.bfloat16)
    gate_grad = (hidden_grad * upper * sig * (1.0 + gate * (1.0 - sig))).astype(jnp.bfloat16)
    slot_grad = jnp.dot(gate_grad, w_gate, preferred_element_type=jnp.float32) + jnp.dot(up_grad, w_up, preferred_element_type=jnp.float32)
    outer = (((0,), (0,)), ((), ()))
    grad_gate = lax.dot_general(gate_grad, inputs, outer, preferred_element_type=jnp.float32).astype(jnp.bfloat16)
    grad_up = lax.dot_general(up_grad, inputs, outer, preferred_element_type=jnp.float32).astype(jnp.bfloat16)
    grad_down = lax.dot_general(hidden, out_grads, outer, preferred_element_type=jnp.float32).astype(jnp.bfloat16)
    return slot_grad, grad_gate, grad_up, grad_down


def reference(out_grad, combine_logits, expert_out, slot_in, router, w_gate, w_up, w_down):
    token_grad, slot_out_bf = lax.map(lambda items: sequence_part(items, router), (out_grad, combine_logits, expert_out))
    per_expert = (jnp.transpose(slot_in, (1, 0, 2)), jnp.transpose(slot_out_bf, (1, 0, 2)), w_gate, w_up, w_down)
    slot_grad, grad_gate, grad_up, grad_down = lax.map(expert_part, per_expert)
    return token_grad, jnp.transpose(slot_grad, (1, 0, 2)), grad_gate, grad_up, grad_down
```

```python
import functools

import jax
import jax.numpy as jnp
from jax import lax
from jax.experimental import pallas as pl
from jax.experimental.pallas import tpu as pltpu
from jax.sharding import PartitionSpec as P

MESH = pl.DeviceIdType.MESH
BF = jnp.bfloat16
F32 = jnp.float32
NT = (((1,), (1,)), ((), ()))
TN = (((0,), (0,)), ((), ()))


def exchange_kernel(
    og_h, lg_h, eo_h, si_h, rt_h, wg_h, wu_h, wd_h,
    sg_o, x_o, so_o, gu_o, hi_o, ld_o, rt_o,
    og_v, lg_v, wgu_v, wd_v, er_g, si_g, so_g, sb, xr, ss, rs, ps, pr, probs_v,
    load_sem, d2d_sem, rs_s, rs_r, ag_s, ag_r, zs_s, zs_r, xs_s, xs_r, fw_sem, sx_s, sx_r, pp_s, pp_r,
):
    seq = lax.axis_index("seq")
    grp = lax.axis_index("grp")
    chip = seq // 2
    core = lax.rem(seq, 2)
    x = chip // 4
    zh = lax.rem(chip, 4)
    other = seq + 1 - 2 * core

    loads = [
        pltpu.make_async_copy(lg_h, lg_v, load_sem.at[0]),
        pltpu.make_async_copy(og_h, og_v, load_sem.at[1]),
        pltpu.make_async_copy(si_h, si_g.at[grp], load_sem.at[2]),
        pltpu.make_async_copy(eo_h, er_g.at[0, x, zh, core], load_sem.at[3]),
        pltpu.make_async_copy(rt_h, er_g.at[1, x, zh, core], load_sem.at[4]),
        pltpu.make_async_copy(wg_h, wgu_v.at[pl.ds(0, 1024)], load_sem.at[5]),
        pltpu.make_async_copy(wu_h, wgu_v.at[pl.ds(1024, 1024)], load_sem.at[6]),
        pltpu.make_async_copy(wd_h, wd_v, load_sem.at[7]),
    ]
    for load in loads:
        load.start()

    def chip_at(k):
        return lax.rem(chip + k, 16)

    def group_at(k):
        return lax.rem(grp + k, 8)

    def x_at(k):
        return lax.rem(x + k, 4)

    def z_at(k):
        return lax.rem(zh + k, 4)

    barrier = pltpu.get_barrier_semaphore()

    def greet_chip(k, _):
        pl.semaphore_signal(barrier, inc=1, device_id=(2 * chip_at(k) + core, grp), device_id_type=MESH)
        return 0

    def greet_group(k, _):
        pl.semaphore_signal(barrier, inc=1, device_id=(seq, group_at(k)), device_id_type=MESH)
        return 0

    lax.fori_loop(1, 16, greet_chip, 0)
    lax.fori_loop(1, 8, greet_group, 0)
    pl.semaphore_signal(barrier, inc=1, device_id=(other, grp), device_id_type=MESH)

    loads[0].wait()
    logits = lg_v[...]
    top = jnp.max(logits, axis=-1, keepdims=True)
    raised = jnp.exp(logits - top)
    probs = raised / jnp.sum(raised, axis=-1, keepdims=True)
    probs_v[...] = probs
    loads[1].wait()
    share = lax.dot_general(probs.astype(BF), og_v[...], TN, preferred_element_type=F32)
    sb[...] = share.reshape(16, 2, 4, 1024).astype(BF)

    pl.semaphore_wait(barrier, 23)

    def remote(src, dst, send, recv, device):
        return pltpu.make_async_remote_copy(
            src_ref=src, dst_ref=dst, send_sem=send, recv_sem=recv, device_id=device, device_id_type=MESH
        )

    swap = remote(sb.at[:, 1 - core], xr, d2d_sem.at[0], d2d_sem.at[1], (other, grp))
    swap.start()

    def slot_in_copy(k):
        return remote(si_g.at[grp], si_g.at[grp], sx_s.at[k], sx_r.at[k], (seq, group_at(k)))

    def z_copy(k):
        here = er_g.at[:, x, zh, core]
        return remote(here, here, zs_s.at[k], zs_r.at[k], (2 * (4 * x + z_at(k)) + core, grp))

    def x_copy(k):
        here = er_g.at[:, x, :, core]
        return remote(here, here, xs_s.at[k], xs_r.at[k], (2 * (4 * x_at(k) + zh) + core, grp))

    def share_copy(k):
        return remote(ss.at[chip_at(k)], rs.at[k], rs_s.at[k], rs_r.at[k], (2 * chip_at(k) + core, grp))

    def slot_out_copy(k):
        return remote(so_g.at[grp], so_g.at[grp], ag_s.at[k], ag_r.at[k], (seq, group_at(k)))

    def partial_copy(k):
        return remote(ps.at[group_at(k)], pr.at[k], pp_s.at[k], pp_r.at[k], (seq, group_at(k)))

    def each(first, last, copy, act):
        def step(k, _):
            act(copy(k))
            return 0

        lax.fori_loop(first, last, step, 0)

    def start(c):
        c.start()

    def landed(c):
        c.wait_recv()

    def sent(c):
        c.wait_send()

    loads[2].wait()
    each(1, 8, slot_in_copy, start)
    loads[3].wait()
    loads[4].wait()
    each(1, 4, z_copy, start)

    swap.wait_recv()
    ss[...] = (sb[:, core].astype(F32) + xr[...].astype(F32)).astype(BF)
    each(1, 16, share_copy, start)

    each(1, 8, slot_in_copy, landed)
    inputs = si_g[...].astype(F32).reshape(32, 1024).astype(BF)
    x_o[...] = inputs
    loads[5].wait()
    loads[6].wait()
    gate_up = lax.dot_general(inputs, wgu_v[...], NT, preferred_element_type=F32)
    gate = gate_up[:, :1024]
    upper = gate_up[:, 1024:]
    sig = jax.nn.sigmoid(gate)
    row = lax.broadcasted_iota(jnp.int32, (32, 1024), 0)
    column = lax.broadcasted_iota(jnp.int32, (32, 1024), 1)
    mine = lax.rem(row, 4) == column // 256
    swish = gate * sig
    hi_o[...] = jnp.where(mine, swish * upper, 0.0).astype(BF)
    up_factor = jnp.where(mine, swish, 0.0)
    gate_factor = jnp.where(mine, upper * sig * (1.0 + gate * (1.0 - sig)), 0.0)

    each(1, 4, z_copy, landed)
    each(1, 4, x_copy, start)

    each(1, 16, share_copy, landed)
    total = ss[chip].astype(F32)
    for k in range(1, 16):
        total = total + rs[k].astype(F32)
    so_g[grp] = total.astype(BF)
    each(1, 8, slot_out_copy, start)

    each(1, 4, x_copy, landed)
    gathered = er_g.at[:, :, :, core]
    forward = remote(gathered, gathered, fw_sem.at[0], fw_sem.at[1], (other, grp))
    forward.start()

    loads[7].wait()
    each(1, 8, slot_out_copy, landed)
    slot_outs = so_g[...].astype(F32).reshape(32, 1024).astype(BF)
    so_o[...] = slot_outs
    hidden_grad = lax.dot_general(slot_outs, wd_v[...], NT, preferred_element_type=F32)
    gu = jnp.concatenate([hidden_grad * gate_factor, hidden_grad * up_factor], axis=1).astype(BF)
    gu_o[...] = gu
    partial = jnp.dot(gu, wgu_v[...], preferred_element_type=F32)
    ps[...] = partial.reshape(8, 4, 1024).astype(BF)
    each(1, 8, partial_copy, start)

    forward.wait_recv()
    outs = er_g[0].astype(F32).reshape(128, 1024).astype(BF)
    rt_o[...] = er_g[1].astype(F32).reshape(128, 1024).astype(BF)
    weight_grad = lax.dot_general(og_v[...], outs, NT, preferred_element_type=F32)
    weights = probs_v[...]
    centre = jnp.sum(weight_grad * weights, axis=-1, keepdims=True)
    ld_o[...] = (weights * (weight_grad - centre)).astype(BF)

    each(1, 8, partial_copy, landed)
    total = ps[grp].astype(F32)
    for k in range(1, 8):
        total = total + pr[k].astype(F32)
    sg_o[...] = total

    swap.wait_send()
    each(1, 8, slot_in_copy, sent)
    each(1, 4, z_copy, sent)
    each(1, 4, x_copy, sent)
    each(1, 16, share_copy, sent)
    each(1, 8, slot_out_copy, sent)
    forward.wait_send()
    each(1, 8, partial_copy, sent)


def write_kernel(x_r, so_r, gu_r, hi_r, ld_r, rt_r, tg_h, gg_h, gu_h, gd_h, tg_v, out_v, sem):
    copies = []
    inputs = x_r[...]
    slot_outs = so_r[...]
    for e in range(4):
        rows = pl.ds(256 * e, 256)
        for j, (left, right, dst) in enumerate(
            (
                (gu_r[:, 256 * e : 256 * e + 256], inputs, gg_h),
                (gu_r[:, 1024 + 256 * e : 1280 + 256 * e], inputs, gu_h),
                (hi_r[:, 256 * e : 256 * e + 256], slot_outs, gd_h),
            )
        ):
            out_v[j, rows] = lax.dot_general(left, right, TN, preferred_element_type=F32).astype(BF)
            copy = pltpu.make_async_copy(out_v.at[j, rows], dst.at[rows], sem.at[3 * e + j])
            copy.start()
            copies.append(copy)
    tg_v[...] = jnp.dot(ld_r[...], rt_r[...], preferred_element_type=F32).astype(BF)
    copy = pltpu.make_async_copy(tg_v, tg_h, sem.at[12])
    copy.start()
    copies.append(copy)
    for copy in copies:
        copy.wait()


def per_device(out_grad, combine_logits, expert_out, slot_in, router, w_gate, w_up, w_down):
    any_space = pl.BlockSpec(memory_space=pl.ANY)
    vmem = pl.BlockSpec(memory_space=pltpu.VMEM)
    dma = pltpu.SemaphoreType.DMA
    sds = jax.ShapeDtypeStruct
    slot_grad, x, so, gu, hi, ld, rt = pl.pallas_call(
        exchange_kernel,
        out_shape=(
            sds((4, 1024), F32),
            sds((32, 1024), BF),
            sds((32, 1024), BF),
            sds((32, 2048), BF),
            sds((32, 1024), BF),
            sds((216, 128), BF),
            sds((128, 1024), BF),
        ),
        in_specs=[any_space] * 8,
        out_specs=(vmem,) * 7,
        scratch_shapes=[
            pltpu.VMEM((216, 1024), BF),
            pltpu.VMEM((216, 128), F32),
            pltpu.VMEM((2048, 1024), BF),
            pltpu.VMEM((1024, 1024), BF),
            pltpu.VMEM((2, 4, 4, 2, 4, 1024), BF),
            pltpu.VMEM((8, 4, 1024), BF),
            pltpu.VMEM((8, 4, 1024), BF),
            pltpu.VMEM((16, 2, 4, 1024), BF),
            pltpu.VMEM((16, 4, 1024), BF),
            pltpu.VMEM((16, 4, 1024), BF),
            pltpu.VMEM((16, 4, 1024), BF),
            pltpu.VMEM((8, 4, 1024), BF),
            pltpu.VMEM((8, 4, 1024), BF),
            pltpu.VMEM((216, 128), F32),
            dma((8,)),
            dma((2,)),
            dma((16,)),
            dma((16,)),
            dma((8,)),
            dma((8,)),
            dma((4,)),
            dma((4,)),
            dma((4,)),
            dma((4,)),
            dma((2,)),
            dma((8,)),
            dma((8,)),
            dma((8,)),
            dma((8,)),
        ],
        compiler_params=pltpu.CompilerParams(
            collective_id=0, has_side_effects=True, vmem_limit_bytes=24 * 1024 * 1024
        ),
        name="exchange",
    )(
        out_grad[0],
        combine_logits[0],
        expert_out[0],
        slot_in[0],
        router,
        w_gate.reshape(1024, 1024),
        w_up.reshape(1024, 1024),
        w_down.reshape(1024, 1024),
    )
    token_grad, grad_gate, grad_up, grad_down = pl.pallas_call(
        write_kernel,
        out_shape=(
            sds((216, 1024), BF),
            sds((1024, 1024), BF),
            sds((1024, 1024), BF),
            sds((1024, 1024), BF),
        ),
        in_specs=[vmem] * 6,
        out_specs=(any_space,) * 4,
        scratch_shapes=[
            pltpu.VMEM((216, 1024), BF),
            pltpu.VMEM((3, 1024, 1024), BF),
            dma((13,)),
        ],
        compiler_params=pltpu.CompilerParams(vmem_limit_bytes=24 * 1024 * 1024),
        name="write",
    )(x, so, gu, hi, ld, rt)
    shape = w_gate.shape
    return (
        token_grad[None],
        slot_grad[None],
        grad_gate.reshape(shape),
        grad_up.reshape(shape),
        grad_down.reshape(shape),
    )


def solution(mesh):
    return jax.shard_map(
        per_device,
        mesh=mesh,
        in_specs=(
            P("grp", "seq", None),
            P("grp", "seq", None),
            P("grp", "seq", None),
            P("grp", "seq", None),
            P("seq", None),
            P("seq", "grp", None),
            P("seq", "grp", None),
            P("seq", "grp", None),
        ),
        out_specs=(
            P("grp", "seq", None),
            P("grp", "seq", None),
            P("seq", "grp", None),
            P("seq", "grp", None),
            P("seq", "grp", None),
        ),
        check_vma=False,
    )
```

```python
import functools

import jax
import jax.numpy as jnp
from jax import lax
from jax.experimental import pallas as pl
from jax.experimental.pallas import tpu as pltpu
from jax.sharding import PartitionSpec as P

MESH = pl.DeviceIdType.MESH
BF = jnp.bfloat16
F32 = jnp.float32
NT = (((1,), (1,)), ((), ()))
TN = (((0,), (0,)), ((), ()))


def exchange_kernel(
    og_h, lg_h, eo_h, si_h, rt_h, wg_h, wu_h, wd_h,
    gg_o, gu_o, gd_o, tg_o, sg_o,
    og_v, lg_v, wgu_v, wd_v, er_g, si_g, so_g, sb, xr, ss, xb, zp, zb, ps, pr, probs_v, gu_v, hi_v,
    load_sem, swap_sem, rx_s, rx_r, rz_s, rz_r, ag_s, ag_r, zs_s, zs_r, xs_s, xs_r, fw_sem, sx_s, sx_r, pp_s, pp_r,
):
    seq = lax.axis_index("seq")
    grp = lax.axis_index("grp")
    chip = seq // 2
    core = lax.rem(seq, 2)
    x = chip // 4
    zh = lax.rem(chip, 4)
    other = seq + 1 - 2 * core

    loads = [
        pltpu.make_async_copy(lg_h, lg_v, load_sem.at[0]),
        pltpu.make_async_copy(og_h, og_v, load_sem.at[1]),
        pltpu.make_async_copy(si_h, si_g.at[grp], load_sem.at[2]),
        pltpu.make_async_copy(eo_h, er_g.at[0, x, zh, core], load_sem.at[3]),
        pltpu.make_async_copy(rt_h, er_g.at[1, x, zh, core], load_sem.at[4]),
        pltpu.make_async_copy(wg_h, wgu_v.at[pl.ds(0, 1024)], load_sem.at[5]),
        pltpu.make_async_copy(wu_h, wgu_v.at[pl.ds(1024, 1024)], load_sem.at[6]),
        pltpu.make_async_copy(wd_h, wd_v, load_sem.at[7]),
    ]
    for load in loads:
        load.start()

    def group_at(k):
        return lax.rem(grp + k, 8)

    def x_at(k):
        return lax.rem(x + k, 4)

    def z_at(k):
        return lax.rem(zh + k, 4)

    def on_x(k):
        return (2 * (4 * x_at(k) + zh) + core, grp)

    def on_z(k):
        return (2 * (4 * x + z_at(k)) + core, grp)

    def in_group(k):
        return (seq, group_at(k))

    barrier = pltpu.get_barrier_semaphore()

    def greet(device):
        pl.semaphore_signal(barrier, inc=1, device_id=device, device_id_type=MESH)

    for k in (2, 1, 3):
        greet(on_z(k))
    for k in (2, 1, 3):
        greet(on_x(k))
    for k in range(1, 8):
        greet(in_group(k))
    greet((other, grp))

    loads[0].wait()
    logits = lg_v[...]
    top = jnp.max(logits, axis=-1, keepdims=True)
    raised = jnp.exp(logits - top)
    probs = raised / jnp.sum(raised, axis=-1, keepdims=True)
    probs_v[...] = probs
    loads[1].wait()
    share = lax.dot_general(probs.astype(BF), og_v[...], TN, preferred_element_type=F32)
    sb[...] = share.reshape(4, 4, 2, 4, 1024).astype(BF)

    pl.semaphore_wait(barrier, 14)

    def remote(src, dst, send, recv, device):
        return pltpu.make_async_remote_copy(
            src_ref=src, dst_ref=dst, send_sem=send, recv_sem=recv, device_id=device, device_id_type=MESH
        )

    swap = remote(sb.at[:, :, 1 - core], xr, swap_sem.at[0], swap_sem.at[1], (other, grp))
    swap.start()

    slot_in_copies = [
        remote(si_g.at[grp], si_g.at[grp], sx_s.at[k], sx_r.at[k], in_group(k)) for k in range(1, 8)
    ]
    one = er_g.at[:, x, zh, core]
    z_copies = [remote(one, one, zs_s.at[k], zs_r.at[k], on_z(k)) for k in (2, 1, 3)]
    line = er_g.at[:, x, :, core]
    x_copies = [remote(line, line, xs_s.at[k], xs_r.at[k], on_x(k)) for k in (2, 1, 3)]
    plane = er_g.at[:, :, :, core]
    forward = remote(plane, plane, fw_sem.at[0], fw_sem.at[1], (other, grp))
    along_x = {
        k: [
            remote(ss.at[x_at(j), z_at(k)], xb.at[k, j], rx_s.at[k, j], rx_r.at[k, j], on_x(j)) for j in (2, 1, 3)
        ]
        for k in (2, 1, 3, 0)
    }
    along_z = {k: remote(zp.at[k], zb.at[k], rz_s.at[k], rz_r.at[k], on_z(k)) for k in (2, 1, 3)}
    slot_out_copies = [
        remote(so_g.at[grp], so_g.at[grp], ag_s.at[k], ag_r.at[k], in_group(k)) for k in range(1, 8)
    ]
    partial_copies = [
        remote(ps.at[group_at(k)], pr.at[k], pp_s.at[k], pp_r.at[k], in_group(k)) for k in range(1, 8)
    ]

    def start(copies):
        for copy in copies:
            copy.start()

    def landed(copies):
        for copy in copies:
            copy.wait_recv()

    loads[2].wait()
    start(slot_in_copies)
    loads[3].wait()
    loads[4].wait()
    start(z_copies)

    swap.wait_recv()
    ss[...] = (sb[:, :, core].astype(F32) + xr[...].astype(F32)).astype(BF)
    for k in (2, 1, 3, 0):
        start(along_x[k])

    landed(slot_in_copies)
    inputs = si_g[...].astype(F32).reshape(32, 1024).astype(BF)

    for k in (2, 1, 3, 0):
        landed(along_x[k])
        total = ss[x, z_at(k)].astype(F32)
        for j in (1, 2, 3):
            total = total + xb[k, j].astype(F32)
        if k:
            zp[k] = total.astype(BF)
            along_z[k].start()

    landed(z_copies)
    start(x_copies)

    loads[5].wait()
    loads[6].wait()
    gate_up = lax.dot_general(inputs, wgu_v[...], NT, preferred_element_type=F32)
    gate = gate_up[:, :1024]
    upper = gate_up[:, 1024:]
    sig = jax.nn.sigmoid(gate)
    row = lax.broadcasted_iota(jnp.int32, (32, 1024), 0)
    column = lax.broadcasted_iota(jnp.int32, (32, 1024), 1)
    mine = lax.rem(row, 4) == column // 256
    swish = gate * sig
    hi_v[...] = jnp.where(mine, swish * upper, 0.0).astype(BF)
    up_factor = jnp.where(mine, swish, 0.0)
    gate_factor = jnp.where(mine, upper * sig * (1.0 + gate * (1.0 - sig)), 0.0)

    for k in (1, 3, 2):
        along_z[k].wait_recv()
        total = total + zb[k].astype(F32)
    so_g[grp] = total.astype(BF)
    start(slot_out_copies)

    loads[7].wait()
    landed(slot_out_copies)
    slot_outs = so_g[...].astype(F32).reshape(32, 1024).astype(BF)
    hidden_grad = lax.dot_general(slot_outs, wd_v[...], NT, preferred_element_type=F32)
    gu_v[...] = jnp.concatenate([hidden_grad * gate_factor, hidden_grad * up_factor], axis=1).astype(BF)
    partial = jnp.dot(gu_v[...], wgu_v[...], preferred_element_type=F32)
    ps[...] = partial.reshape(8, 4, 1024).astype(BF)
    start(partial_copies)

    landed(x_copies)
    forward.start()

    def outer(left, right, dst, first):
        for e in range(4):
            columns = pl.ds(first + 256 * e, 256)
            dst[pl.ds(256 * e, 256)] = lax.dot_general(
                left[:, columns], right, TN, preferred_element_type=F32
            ).astype(BF)

    outer(gu_v, inputs, gg_o, 0)
    outer(gu_v, inputs, gu_o, 1024)
    outer(hi_v, slot_outs, gd_o, 0)

    forward.wait_recv()
    outs = er_g[0].astype(F32).reshape(128, 1024).astype(BF)
    routes = er_g[1].astype(F32).reshape(128, 1024).astype(BF)
    weight_grad = lax.dot_general(og_v[...], outs, NT, preferred_element_type=F32)
    weights = probs_v[...]
    centre = jnp.sum(weight_grad * weights, axis=-1, keepdims=True)
    logit_grad = (weights * (weight_grad - centre)).astype(BF)
    tg_o[...] = jnp.dot(logit_grad, routes, preferred_element_type=F32).astype(BF)

    landed(partial_copies)
    total = ps[grp].astype(F32)
    for k in range(1, 8):
        total = total + pr[k].astype(F32)
    sg_o[...] = total

    sends = [swap, forward, *slot_in_copies, *z_copies, *x_copies, *along_z.values(), *slot_out_copies]
    for copy in sends + partial_copies + [copy for k in (2, 1, 3, 0) for copy in along_x[k]]:
        copy.wait_send()


def write_kernel(*refs):
    sources, outs, sem = refs[:5], refs[5:10], refs[10]
    copies = [pltpu.make_async_copy(sources[i], outs[i], sem.at[i]) for i in range(5)]
    for copy in copies:
        copy.start()
    for copy in copies:
        copy.wait()


def per_device(out_grad, combine_logits, expert_out, slot_in, router, w_gate, w_up, w_down):
    any_space = pl.BlockSpec(memory_space=pl.ANY)
    vmem = pl.BlockSpec(memory_space=pltpu.VMEM)
    dma = pltpu.SemaphoreType.DMA
    outs = [
        ((1024, 1024), BF),
        ((1024, 1024), BF),
        ((1024, 1024), BF),
        ((216, 1024), BF),
        ((4, 1024), F32),
    ]
    arguments = [
        out_grad[0],
        combine_logits[0],
        expert_out[0],
        slot_in[0],
        router,
        w_gate.reshape(1024, 1024),
        w_up.reshape(1024, 1024),
        w_down.reshape(1024, 1024),
    ]
    block = (4, 1024)
    results = pl.pallas_call(
        exchange_kernel,
        out_shape=[pltpu.VMEM(shape, kind) for shape, kind in outs],
        in_specs=[any_space] * 8,
        out_specs=[vmem] * 5,
        scratch_shapes=[
            pltpu.VMEM((216, 1024), BF),
            pltpu.VMEM((216, 128), F32),
            pltpu.VMEM((2048, 1024), BF),
            pltpu.VMEM((1024, 1024), BF),
            pltpu.VMEM((2, 4, 4, 2, *block), BF),
            pltpu.VMEM((8, *block), BF),
            pltpu.VMEM((8, *block), BF),
            pltpu.VMEM((4, 4, 2, *block), BF),
            pltpu.VMEM((4, 4, *block), BF),
            pltpu.VMEM((4, 4, *block), BF),
            pltpu.VMEM((4, 4, *block), BF),
            pltpu.VMEM((4, *block), BF),
            pltpu.VMEM((4, *block), BF),
            pltpu.VMEM((8, *block), BF),
            pltpu.VMEM((8, *block), BF),
            pltpu.VMEM((216, 128), F32),
            pltpu.VMEM((32, 2048), BF),
            pltpu.VMEM((32, 1024), BF),
            dma((8,)),
            dma((2,)),
            dma((4, 4)),
            dma((4, 4)),
            dma((4,)),
            dma((4,)),
            dma((8,)),
            dma((8,)),
            dma((4,)),
            dma((4,)),
            dma((4,)),
            dma((4,)),
            dma((2,)),
            dma((8,)),
            dma((8,)),
            dma((8,)),
            dma((8,)),
        ],
        compiler_params=pltpu.CompilerParams(
            collective_id=0, has_side_effects=True, vmem_limit_bytes=16 * 1024 * 1024
        ),
        name="exchange",
    )(*[pltpu.with_memory_space_constraint(argument, pltpu.HBM) for argument in arguments])
    grad_gate, grad_up, grad_down, token_grad, slot_grad = pl.pallas_call(
        write_kernel,
        out_shape=[jax.ShapeDtypeStruct(shape, kind) for shape, kind in outs],
        in_specs=[vmem] * 5,
        out_specs=[any_space] * 5,
        scratch_shapes=[dma((5,))],
        compiler_params=pltpu.CompilerParams(vmem_limit_bytes=1024 * 1024),
        name="write",
    )(*results)
    shape = w_gate.shape
    return (
        token_grad[None],
        slot_grad[None],
        grad_gate.reshape(shape),
        grad_up.reshape(shape),
        grad_down.reshape(shape),
    )


def solution(mesh):
    return jax.shard_map(
        per_device,
        mesh=mesh,
        in_specs=(
            P("grp", "seq", None),
            P("grp", "seq", None),
            P("grp", "seq", None),
            P("grp", "seq", None),
            P("seq", None),
            P("seq", "grp", None),
            P("seq", "grp", None),
            P("seq", "grp", None),
        ),
        out_specs=(
            P("grp", "seq", None),
            P("grp", "seq", None),
            P("seq", "grp", None),
            P("seq", "grp", None),
            P("seq", "grp", None),
        ),
        check_vma=False,
    )
```
